32 devices in a mesh: grp: 2 (over y), lay: 4 (over z), wid: 2 (over x), rep: 2 (over core).
Axes of the slice: x: 2, y: 2, z: 4, core: 2. Of those that a mesh axis runs over, the one named last changes fastest.
Arguments:
- acts: bfloat16 [4, 1024, 2048], P(None, ('grp', 'rep'), 'wid'), parts along dimension 1, may hold values from -6 to 6
- targets: bfloat16 [4, 1024, 2048], P(None, ('grp', 'rep'), 'wid'), parts along dimension 1, may hold values from -6 to 6
- enc_weight: bfloat16 [2048, 8192], P('wid', 'lay'), may hold values from -0.125 to 0.125
- enc_bias: float32 [8192], P('lay'), may hold values from -3 to 3
- gate_mask: int32 [1024, 32], P(('grp', 'rep'), 'lay'), parts along dimension 0, may hold values 0 or 1
- dec_list: int32 [84, 3], P('lay'), may hold values from -1 to 7, as said below
- dec_weight: bfloat16 [84, 256, 2048], P('lay', None, 'wid'), may hold values from -0.125 to 0.125
Outputs:
- grad_enc: float32 [4096, 8192], P(('grp', 'wid'), ('lay', 'rep')), parts along dimension 0
- grad_bias: float32 [16384], P(('grp', 'lay', 'rep')), parts along dimension 0
- grad_dec: float32 [168, 256, 2048], P(('grp', 'lay'), 'rep', 'wid'), parts along dimension 0
The draws below stay inside these ranges and needn't reach their ends.
There are 2 independent parts, one for each index of `grp`. The reference program is written for one: setup_inputs(seed, part) draws one part's arguments, and reference() takes and returns one part's arrays. A program takes and returns all parts, laid end to end along the dimension named above; an argument that names none is the same for every part. Nothing has to cross between parts.
Inputs may be any that keep to these rules, and one draw needn't show every extreme that they name: `dec_list`: each row is (source layer, target layer, latent block within the layer's slab); every triple with source <= target < 4 and block < 8 stands in exactly one row; every other row is (-1, -1, -1).
All inputs are finite; a program needn't handle non-finite values. No bound on the sum of `gate_mask` on one device may be relied on, other than what follows from the above.
Results may differ from the reference program's by a relative error of at most 0.019.
Values may be sent and summed in bfloat16 or wider, within the bound.
A program may use at most 128 MiB of HBM per device.

```python
import jax
import jax.numpy as jnp
import numpy as np
from jax import lax

D = 2048
F = 2048
L = 4
BLK = 256
TOKENS = 512
NLB = 32
SLOTS = 21
N_LAY = 4


def draw_dec_list(key, part):
    blocks_layer = F // BLK
    triples = np.array([[source_layer, target_layer, within] for source_layer in range(L) for target_layer in range(source_layer, L) for within in range(blocks_layer)], dtype=np.int32)
    placing = jax.random.permutation(jax.random.fold_in(key, 11), N_LAY * SLOTS)
    filled = jnp.full((N_LAY * SLOTS, 3), -1, jnp.int32)
    return filled.at[placing[:triples.shape[0]]].set(jnp.asarray(triples))


def with_ends(values, own_key, least, largest):
    index_at = [jax.random.randint(jax.random.fold_in(own_key, axis), (), 0, length) for axis, length in enumerate(values.shape)]
    widest = values.shape.index(max(values.shape))
    beside = index_at[:widest] + [(index_at[widest] + 1) % values.shape[widest]] + index_at[widest + 1:]
    return values.at[tuple(index_at)].set(least).at[tuple(beside)].set(largest)


def levels(rng, shape, shards, low, largest):
    def one(axis_at, parts):
        steps = jax.random.uniform(jax.random.fold_in(jax.random.fold_in(rng, 6), axis_at), (parts,), jnp.float32, low / len(shards), largest / len(shards))
        return jnp.repeat(jnp.exp(steps), shape[axis_at] // parts).reshape((-1,) + (1,) * (len(shape) - axis_at - 1))

    loudness = one(*shards[0])
    for cut in shards[1:]:
        loudness = loudness * one(*cut)
    return loudness


def bell_draw(key, shape, scale, limit, pieces=(), kind=jnp.bfloat16):
    level = levels(key, shape, pieces, -0.22, 0.18) if pieces else 1.0
    drawn = jax.random.normal(key, shape, jnp.float32) * scale * level
    return jnp.minimum(jnp.maximum(drawn, -limit), limit).astype(kind)


def setup_inputs(seed: int = 0, part: int = 0) -> dict:
    keys = jax.random.split(jax.random.key(seed), 8)
    part_keys = jax.random.split(jax.random.fold_in(keys[7], part), 8)
    return {
        "acts": bell_draw(part_keys[0], (L, TOKENS, D), 1.0, 6.0, ((1, 2), (2, 2))),
        "targets": bell_draw(part_keys[1], (L, TOKENS, D), 1.0, 6.0, ((1, 2), (2, 2))),
        "enc_weight": bell_draw(keys[2], (D, L * F), D ** -0.5, 0.125, ((0, 2), (1, 4))),
        "enc_bias": bell_draw(keys[3], (L * F,), 0.5, 3.0, ((0, 4),), jnp.float32),
        "gate_mask": with_ends((jax.random.randint(part_keys[4], (TOKENS, NLB), 0, 2) < 1).astype(jnp.int32), jax.random.fold_in(part_keys[4], 1), 0, 1),
        "dec_list": draw_dec_list(jax.random.fold_in(keys[7], 71), part),
        "dec_weight": bell_draw(keys[6], (N_LAY * SLOTS, BLK, D), F ** -0.5, 0.125, ((0, 4), (2, 2))),
    }


ROOT = 0.7978845608028654
CUBIC = 0.044715


def smooth_gate(shifted):
    inside_arg = ROOT * (shifted + CUBIC * shifted * shifted * shifted)
    return 0.5 * shifted * (1.0 + jnp.tanh(inside_arg))


def gate_slope(shifted):
    inside_arg = ROOT * (shifted + CUBIC * shifted * shifted * shifted)
    tanh_part = jnp.tanh(inside_arg)
    return 0.5 * (1.0 + tanh_part) + 0.5 * shifted * (1.0 - tanh_part * tanh_part) * ROOT * (1.0 + 3.0 * CUBIC * shifted * shifted)


def slot_tables(slot_entry, blocks_layer, blocks_total):
    block_id = slot_entry[:, 0] * blocks_layer + slot_entry[:, 2]
    target_layer = slot_entry[:, 1]
    slot_valid = (target_layer >= 0).astype(jnp.float32)
    target_hot = (target_layer[:, None] == jnp.arange(L, dtype=jnp.int32)[None, :]).astype(jnp.float32)
    block_hot = (block_id[:, None] == jnp.arange(blocks_total, dtype=jnp.int32)[None, :]).astype(jnp.float32)
    return block_id, target_layer, slot_valid, target_hot, block_hot


def reference(acts, targets, enc_weight, enc_bias, gate_mask, dec_list, dec_weight):
    blocks_layer = F // BLK
    blocks_total = L * blocks_layer
    tokens = acts.shape[1]
    pre_act = jnp.concatenate([jnp.dot(acts[layer_index], enc_weight[:, layer_index * F:(layer_index + 1) * F], preferred_element_type=jnp.float32) for layer_index in range(L)], axis=1)
    shifted = (pre_act + enc_bias.astype(jnp.float32)[None, :]).reshape(tokens, blocks_total, BLK)
    keep_mask = gate_mask.astype(jnp.float32)[:, :, None]
    latent = (smooth_gate(shifted) * keep_mask).astype(jnp.bfloat16)
    lists = dec_list.reshape(N_LAY, SLOTS, 3)
    weights = dec_weight.reshape(N_LAY, SLOTS, BLK, D)

    def forward_step(running, slot_pair):
        slot_entry, weight = slot_pair
        block_id, target_layer, slot_valid, target_hot, block_hot = slot_tables(slot_entry, blocks_layer, blocks_total)
        slot_lat = jnp.take(latent, jnp.maximum(block_id, 0), axis=1).astype(jnp.float32)
        contrib = jnp.einsum('tkb,kbd->ktd', slot_lat, weight.astype(jnp.float32), precision=lax.Precision.HIGHEST)
        return running + jnp.einsum('kl,ktd->ltd', target_hot, contrib, precision=lax.Precision.HIGHEST), None

    recon, _ = lax.scan(forward_step, jnp.zeros((L, tokens, D), jnp.float32), (lists, weights))
    scaled_error = ((recon - targets.astype(jnp.float32)) * (tokens ** -0.5)).astype(jnp.bfloat16)

    def backward_step(running, slot_pair):
        slot_entry, weight = slot_pair
        block_id, target_layer, slot_valid, target_hot, block_hot = slot_tables(slot_entry, blocks_layer, blocks_total)
        slot_lat = jnp.take(latent, jnp.maximum(block_id, 0), axis=1).astype(jnp.float32)
        err_slot = jnp.take(scaled_error, jnp.maximum(target_layer, 0), axis=0).astype(jnp.float32)
        dec_grad = jnp.einsum('tkb,ktd->kbd', slot_lat, err_slot, precision=lax.Precision.HIGHEST) * slot_valid[:, None, None]
        slot_error = jnp.einsum('ktd,kbd->tkb', err_slot, weight.astype(jnp.float32), precision=lax.Precision.HIGHEST)
        outgoing = jnp.einsum('tkb,kg->tgb', slot_error, block_hot, precision=lax.Precision.HIGHEST).astype(jnp.bfloat16)
        return running + outgoing.astype(jnp.float32), dec_grad

    latent_error, dec_grads = lax.scan(backward_step, jnp.zeros((tokens, blocks_total, BLK), jnp.float32), (lists, weights))
    pre_grad = (latent_error * keep_mask * gate_slope(shifted)).astype(jnp.bfloat16).reshape(tokens, L * F)
    grad_enc = jnp.concatenate([jnp.dot(acts[layer_index].T, pre_grad[:, layer_index * F:(layer_index + 1) * F], preferred_element_type=jnp.float32) for layer_index in range(L)], axis=1)
    grad_bias = jnp.sum(pre_grad.astype(jnp.float32), axis=0)
    grad_dec = dec_grads.reshape(N_LAY * SLOTS, BLK, D)
    return grad_enc, grad_bias, grad_dec
```

```python
import jax
import jax.numpy as jnp
from jax import lax
from jax.experimental import pallas as pl
from jax.experimental.pallas import tpu as pltpu
from jax.sharding import PartitionSpec as P

ROOT = 0.7978845608028654
CUBIC = 0.044715
MESH = pl.DeviceIdType.MESH
BF16 = jnp.bfloat16
F32 = jnp.float32


def smooth_gate(shifted):
    inside_arg = ROOT * (shifted + CUBIC * shifted * shifted * shifted)
    return 0.5 * shifted * (1.0 + jnp.tanh(inside_arg))


def gate_slope(shifted):
    inside_arg = ROOT * (shifted + CUBIC * shifted * shifted * shifted)
    tanh_part = jnp.tanh(inside_arg)
    return 0.5 * (1.0 + tanh_part) + 0.5 * shifted * (1.0 - tanh_part * tanh_part) * ROOT * (
        1.0 + 3.0 * CUBIC * shifted * shifted
    )


def loop(first, count, step):
    if count <= 4:
        for d in range(first, count):
            step(d)
    else:
        lax.fori_loop(first, count, lambda d, c: (step(d), c)[1], 0)


def others(me, count, step):
    loop(1, count, lambda d: step(lax.rem(me + d, count)))


def signal(barrier, **where):
    pl.semaphore_signal(barrier, inc=1, device_id=where, device_id_type=MESH)


def remote(src, dst, send_sem, recv_sem, **where):
    return pltpu.make_async_remote_copy(
        src_ref=src, dst_ref=dst, send_sem=send_sem, recv_sem=recv_sem, device_id=where,
        device_id_type=MESH,
    )


ANY = pl.BlockSpec(memory_space=pl.ANY)


def comm(body, args, outs, sems, cid):
    return pl.pallas_call(
        body,
        out_shape=tuple(outs),
        in_specs=[ANY] * len(args),
        out_specs=tuple([ANY] * len(outs)),
        scratch_shapes=[pltpu.SemaphoreType.DMA((s,)) for s in sems],
        compiler_params=pltpu.CompilerParams(collective_id=cid, has_side_effects=True),
        name=f"exchange_{cid}",
    )(*args)


def exchange(axis, x, out_shape, src_of, dst_of, cid):
    n = lax.axis_size(axis)

    def body(x_ref, o_ref, ssem, rsem, lsem):
        me = lax.axis_index(axis)
        barrier = pltpu.get_barrier_semaphore()
        others(me, n, lambda j: signal(barrier, **{axis: j}))
        pl.semaphore_wait(barrier, n - 1)

        def send(j):
            return remote(
                src_of(x_ref, j), dst_of(o_ref, me), ssem.at[j], rsem.at[me], **{axis: j}
            )

        def arrival(j):
            return remote(
                src_of(x_ref, me), dst_of(o_ref, j), ssem.at[j], rsem.at[j], **{axis: j}
            )

        others(me, n, lambda j: send(j).start())
        own = pltpu.make_async_copy(src_of(x_ref, me), dst_of(o_ref, me), lsem.at[0])
        own.start()
        others(me, n, lambda j: arrival(j).wait_recv())
        others(me, n, lambda j: send(j).wait_send())
        own.wait()

    return comm(body, [x], [jax.ShapeDtypeStruct(out_shape, x.dtype)], (n, n, 1), cid)[0]


def gather_latents(h, cid):
    n, w_count = lax.axis_size("lay"), lax.axis_size("wid")
    blocks, toks, width = h.shape

    def body(h_ref, o_ref, zs, zr, xs, xr, lsem):
        l, w = lax.axis_index("lay"), lax.axis_index("wid")
        barrier = pltpu.get_barrier_semaphore()
        others(l, n, lambda j: signal(barrier, lay=j))
        others(w, w_count, lambda v: signal(barrier, wid=v))
        pl.semaphore_wait(barrier, n + w_count - 2)

        def slot(j, v):
            return o_ref.at[pl.ds(j * blocks, blocks), v]

        def z_copy(j, source):
            return remote(h_ref, slot(source, w), zs.at[j], zr.at[source], lay=j)

        def x_own(v):
            return remote(h_ref, slot(l, w), xs.at[l * w_count + v], xr.at[l * w_count + w], wid=v)

        def x_copy(j, v, source):
            return remote(
                slot(j, source), slot(j, source), xs.at[j * w_count + v],
                xr.at[j * w_count + source], wid=v,
            )

        def nearest(step):
            def both(d):
                for j in (l - d, l + d):
                    @pl.when((j >= 0) & (j < n))
                    def _():
                        step(j)
            loop(1, n, both)

        others(w, w_count, lambda v: x_own(v).start())
        nearest(lambda j: z_copy(j, l).start())
        own = pltpu.make_async_copy(h_ref, slot(l, w), lsem.at[0])
        own.start()

        def forward(j):
            z_copy(j, j).wait_recv()
            others(w, w_count, lambda v: x_copy(j, v, w).start())

        nearest(forward)
        others(w, w_count, lambda v: x_own(v).wait_send())
        nearest(lambda j: z_copy(j, l).wait_send())
        nearest(lambda j: others(w, w_count, lambda v: x_copy(j, v, w).wait_send()))
        loop(0, n, lambda j: others(w, w_count, lambda v: x_copy(j, v, v).wait_recv()))
        own.wait()

    out = jax.ShapeDtypeStruct((n * blocks, w_count, toks, width), h.dtype)
    return comm(body, [h], [out], (n, n, n * w_count, n * w_count, 1), cid)[0]


def slots_and_twin(slot_err, lat, err, acts_here, cid):
    w_count, r_count = lax.axis_size("wid"), lax.axis_size("rep")
    assert r_count == 2
    slots, _, toks, width = slot_err.shape
    half = width // r_count

    def body(s_ref, l_ref, e_ref, a_ref, so_ref, lo_ref, eo_ref, ao_ref, ssem, rsem, lsem, ts, tr):
        w, r = lax.axis_index("wid"), lax.axis_index("rep")
        twin = 1 - r
        barrier = pltpu.get_barrier_semaphore()
        others(w, w_count, lambda v: signal(barrier, wid=v))
        signal(barrier, rep=twin)
        pl.semaphore_wait(barrier, w_count)

        def send(v):
            return remote(s_ref.at[:, v], so_ref.at[w], ssem.at[v], rsem.at[w], wid=v)

        def arrival(v):
            return remote(s_ref.at[:, w], so_ref.at[v], ssem.at[v], rsem.at[v], wid=v)

        others(w, w_count, lambda v: send(v).start())
        twins = [
            remote(l_ref.at[:, :, pl.ds(pl.multiple_of(twin * half, half), half)], lo_ref,
                   ts.at[0], tr.at[0], rep=twin),
            remote(e_ref, eo_ref, ts.at[1], tr.at[1], rep=twin),
            remote(a_ref, ao_ref, ts.at[2], tr.at[2], rep=twin),
        ]
        for c in twins:
            c.start()
        own = pltpu.make_async_copy(s_ref.at[:, w], so_ref.at[w], lsem.at[0])
        own.start()
        others(w, w_count, lambda v: arrival(v).wait_recv())
        others(w, w_count, lambda v: send(v).wait_send())
        own.wait()
        for c in twins:
            c.wait()

    outs = [
        jax.ShapeDtypeStruct((w_count, slots, toks, width), slot_err.dtype),
        jax.ShapeDtypeStruct(lat.shape[:2] + (half,), lat.dtype),
        jax.ShapeDtypeStruct(err.shape, err.dtype),
        jax.ShapeDtypeStruct(acts_here.shape, acts_here.dtype),
    ]
    return comm(body, [slot_err, lat, err, acts_here], outs, (w_count, w_count, 1, 3, 3), cid)


def gather_pre_grad(pg, cid):
    w_count, r_count = lax.axis_size("wid"), lax.axis_size("rep")
    _, toks, columns = pg.shape

    def body(p_ref, o_ref, ssem, rsem, lsem):
        w, r = lax.axis_index("wid"), lax.axis_index("rep")
        barrier = pltpu.get_barrier_semaphore()

        def peers(step):
            others(w, w_count, lambda v: loop(0, r_count, lambda q: step(v, q)))
            others(r, r_count, lambda q: step(w, q))

        peers(lambda v, q: signal(barrier, wid=v, rep=q))
        pl.semaphore_wait(barrier, w_count * r_count - 1)

        def send(v, q):
            return remote(p_ref.at[q], o_ref.at[r, w], ssem.at[q * w_count + v],
                          rsem.at[r * w_count + w], wid=v, rep=q)

        def arrival(v, q):
            return remote(p_ref.at[q], o_ref.at[q, v], ssem.at[q * w_count + v],
                          rsem.at[q * w_count + v], wid=v, rep=q)

        peers(lambda v, q: send(v, q).start())
        own = pltpu.make_async_copy(p_ref.at[r], o_ref.at[r, w], lsem.at[0])
        own.start()
        peers(lambda v, q: arrival(v, q).wait_recv())
        peers(lambda v, q: send(v, q).wait_send())
        own.wait()

    out = jax.ShapeDtypeStruct((r_count, w_count, toks, columns), pg.dtype)
    total = w_count * r_count
    return comm(body, [pg], [out], (total, total, 1), cid)[0]


def slot_call(body, tables, args, in_specs, out_shape, out_spec, scratch, flops, name):
    moved = sum(a.size * a.dtype.itemsize for a in args) + out_shape.size * out_shape.dtype.itemsize
    return pl.pallas_call(
        body,
        out_shape=out_shape,
        grid_spec=pltpu.PrefetchScalarGridSpec(
            num_scalar_prefetch=len(tables), grid=(tables[0].shape[0],), in_specs=in_specs,
            out_specs=out_spec, scratch_shapes=scratch,
        ),
        compiler_params=pltpu.CompilerParams(vmem_limit_bytes=48 * 1024 * 1024),
        cost_estimate=pl.CostEstimate(flops=flops, bytes_accessed=moved, transcendentals=0),
        name=name,
    )(*tables, *args)


def decode(ids, tgt, valid, lat, dec_weight, layers):
    slots, block, width = dec_weight.shape
    toks = lat.shape[1]

    def body(i_ref, t_ref, v_ref, lat_ref, w_ref, o_ref, acc):
        k = pl.program_id(0)

        @pl.when(k == 0)
        def _():
            acc[...] = jnp.zeros_like(acc)

        @pl.when(v_ref[k] > 0)
        def _():
            acc[t_ref[k]] += jnp.dot(lat_ref[0], w_ref[0], preferred_element_type=F32)

        @pl.when(k == slots - 1)
        def _():
            o_ref[...] = acc[...].astype(o_ref.dtype)

    return slot_call(
        body, (ids, tgt, valid), (lat, dec_weight),
        [pl.BlockSpec((1, toks, block), lambda k, i, t, v: (i[k], 0, 0)),
         pl.BlockSpec((1, block, width), lambda k, i, t, v: (k, 0, 0))],
        jax.ShapeDtypeStruct((layers, toks, width), BF16),
        pl.BlockSpec((layers, toks, width), lambda k, i, t, v: (0, 0, 0)),
        [pltpu.VMEM((layers, toks, width), F32)], 2 * slots * toks * block * width, "decode",
    )


def slot_errors(tgt, err, dec_weight):
    slots, block, width = dec_weight.shape
    layers, toks, _ = err.shape

    def body(t_ref, e_ref, w_ref, o_ref):
        k = pl.program_id(0)
        o_ref[0] = lax.dot_general(
            e_ref[t_ref[k]], w_ref[0], (((1,), (1,)), ((), ())), preferred_element_type=F32
        ).astype(o_ref.dtype)

    return slot_call(
        body, (tgt,), (err, dec_weight),
        [pl.BlockSpec((layers, toks, width), lambda k, t: (0, 0, 0)),
         pl.BlockSpec((1, block, width), lambda k, t: (k, 0, 0))],
        jax.ShapeDtypeStruct((slots, toks, block), BF16),
        pl.BlockSpec((1, toks, block), lambda k, t: (k, 0, 0)),
        [], 2 * slots * toks * block * width, "slot_errors",
    )


def combine(ids, valid, parts, blocks_total):
    w_count, slots, toks, block = parts.shape

    def body(i_ref, v_ref, p_ref, o_ref, acc):
        k = pl.program_id(0)

        @pl.when(k == 0)
        def _():
            acc[...] = jnp.zeros_like(acc)

        @pl.when(v_ref[k] > 0)
        def _():
            acc[i_ref[k]] += jnp.sum(p_ref[:, 0].astype(F32), axis=0)

        @pl.when(k == slots - 1)
        def _():
            o_ref[...] = acc[...].astype(o_ref.dtype)

    return slot_call(
        body, (ids, valid), (parts,),
        [pl.BlockSpec((w_count, 1, toks, block), lambda k, i, v: (0, k, 0, 0))],
        jax.ShapeDtypeStruct((blocks_total, toks, block), BF16),
        pl.BlockSpec((blocks_total, toks, block), lambda k, i, v: (0, 0, 0)),
        [pltpu.VMEM((blocks_total, toks, block), F32)], w_count * slots * toks * block, "combine",
    )


def decoder_grads(ids, tgt, valid, rep, lat, lat_twin, err, err_twin, slots):
    layers, toks, width = err.shape
    half = lat_twin.shape[2]

    def body(i_ref, t_ref, v_ref, r_ref, l_ref, lt_ref, e_ref, et_ref, o_ref):
        k = pl.program_id(0)
        over = (((0,), (0,)), ((), ()))

        @pl.when(v_ref[k] > 0)
        def _():
            t = t_ref[k]
            o_ref[0] = lax.dot_general(
                l_ref[0], e_ref[t], over, preferred_element_type=F32
            ) + lax.dot_general(lt_ref[0], et_ref[t], over, preferred_element_type=F32)

        @pl.when(v_ref[k] == 0)
        def _():
            o_ref[...] = jnp.zeros_like(o_ref)

    return slot_call(
        body, (ids, tgt, valid, rep), (lat, lat_twin, err, err_twin),
        [pl.BlockSpec((1, toks, half), lambda k, i, t, v, r: (i[k], 0, r[0])),
         pl.BlockSpec((1, toks, half), lambda k, i, t, v, r: (i[k], 0, 0)),
         pl.BlockSpec((layers, toks, width), lambda k, i, t, v, r: (0, 0, 0)),
         pl.BlockSpec((layers, toks, width), lambda k, i, t, v, r: (0, 0, 0))],
        jax.ShapeDtypeStruct((slots, half, width), F32),
        pl.BlockSpec((1, half, width), lambda k, i, t, v, r: (k, 0, 0)),
        [], 4 * slots * toks * half * width, "decoder_grads",
    )


def local(acts, targets, enc_weight, enc_bias, gate_mask, dec_list, dec_weight):
    layers, tok_rows, width_part = acts.shape
    lat_dev = enc_weight.shape[1]
    slots, block, _ = dec_weight.shape
    per_dev = lat_dev // block
    n, w_count, r_count = lax.axis_size("lay"), lax.axis_size("wid"), lax.axis_size("rep")
    lay, wid, rep = lax.axis_index("lay"), lax.axis_index("wid"), lax.axis_index("rep")
    lat_total = lat_dev * n
    blocks_total = lat_total // block
    latents_layer = lat_total // layers
    blocks_layer = latents_layer // block
    toks = tok_rows // w_count
    rows = tok_rows // n

    tgt = dec_list[:, 1]
    valid = (tgt >= 0).astype(jnp.int32)
    ids = jnp.maximum(dec_list[:, 0] * blocks_layer + dec_list[:, 2], 0)
    tgt = jnp.maximum(tgt, 0)

    here = lax.dynamic_index_in_dim(acts, lay * lat_dev // latents_layer, 0, keepdims=False)
    partial = jnp.dot(here, enc_weight, preferred_element_type=F32).astype(BF16)
    parts = exchange(
        "wid", partial.reshape(w_count, toks, lat_dev), (w_count, toks, lat_dev),
        lambda x, j: x.at[j], lambda o, j: o.at[j], 0,
    )
    shifted = jnp.sum(parts.astype(F32), axis=0) + enc_bias[None, :]
    shifted = shifted.reshape(toks, per_dev, block).transpose(1, 0, 2)
    keep = lax.dynamic_slice_in_dim(gate_mask, wid * toks, toks, 0).astype(F32).T[:, :, None]
    latent = (smooth_gate(shifted) * keep).astype(BF16)
    lat = gather_latents(latent, 1).reshape(blocks_total, tok_rows, block)

    recon_part = decode(ids, tgt, valid, lat, dec_weight, layers)
    recon_in = exchange(
        "lay", recon_part.reshape(layers, n, rows, width_part), (n, layers, rows, width_part),
        lambda x, j: x.at[:, j], lambda o, j: o.at[j], 2,
    )
    recon = jnp.sum(recon_in.astype(F32), axis=0)
    own_target = lax.dynamic_slice_in_dim(targets, lay * rows, rows, 1)
    scale = float(tok_rows * r_count) ** (-0.5)
    own_err = ((recon - own_target.astype(F32)) * scale).astype(BF16)
    err = exchange(
        "lay", own_err, (layers, n, rows, width_part),
        lambda x, j: x, lambda o, j: o.at[:, j], 3,
    ).reshape(layers, tok_rows, width_part)

    slot_err = slot_errors(tgt, err, dec_weight).reshape(slots, w_count, toks, block)
    slot_in, lat_twin, err_twin, acts_twin = slots_and_twin(slot_err, lat, err, here, 4)
    outgoing = combine(ids, valid, slot_in, blocks_total)
    incoming = exchange(
        "lay", outgoing.reshape(n, per_dev, toks, block), (n, per_dev, toks, block),
        lambda x, j: x.at[j], lambda o, j: o.at[j], 5,
    )
    dec_out = decoder_grads(
        ids, tgt, valid, rep.reshape(1).astype(jnp.int32), lat, lat_twin, err, err_twin, slots
    )
    latent_error = jnp.sum(incoming.astype(F32), axis=0)
    pre_grad = (latent_error * keep * gate_slope(shifted)).astype(BF16)
    columns = lat_dev // r_count
    pre_grad = pre_grad.transpose(1, 0, 2).reshape(toks, r_count, columns).transpose(1, 0, 2)
    pre_all = gather_pre_grad(pre_grad, 6).reshape(r_count, tok_rows, columns)

    mine = lax.dynamic_index_in_dim(pre_all, rep, 0, keepdims=False)
    theirs = lax.dynamic_index_in_dim(pre_all, 1 - rep, 0, keepdims=False)
    over = (((0,), (0,)), ((), ()))
    enc_out = lax.dot_general(
        jnp.concatenate([here, acts_twin], 0), jnp.concatenate([mine, theirs], 0), over,
        preferred_element_type=F32,
    )
    bias_out = jnp.sum(pre_all.astype(F32), axis=(0, 1))
    return (enc_out, bias_out, dec_out)


def solution(mesh):
    return jax.shard_map(
        local,
        mesh=mesh,
        in_specs=(
            P(None, ("grp", "rep"), "wid"),
            P(None, ("grp", "rep"), "wid"),
            P("wid", "lay"),
            P("lay"),
            P(("grp", "rep"), "lay"),
            P("lay", None),
            P("lay", None, "wid"),
        ),
        out_specs=(
            P(("grp", "wid"), ("lay", "rep")),
            P(("grp", "lay", "rep")),
            P(("grp", "lay"), "rep", "wid"),
        ),
        check_vma=False,
    )
```

```python
import jax
import jax.numpy as jnp
from jax import lax
from jax.experimental import pallas as pl
from jax.experimental.pallas import tpu as pltpu
from jax.sharding import PartitionSpec as P

ROOT = 0.7978845608028654
CUBIC = 0.044715
MESH = pl.DeviceIdType.MESH
BF16 = jnp.bfloat16
F32 = jnp.float32


def smooth_gate(shifted):
    inside_arg = ROOT * (shifted + CUBIC * shifted * shifted * shifted)
    return 0.5 * shifted * (1.0 + jnp.tanh(inside_arg))


def gate_slope(shifted):
    inside_arg = ROOT * (shifted + CUBIC * shifted * shifted * shifted)
    tanh_part = jnp.tanh(inside_arg)
    return 0.5 * (1.0 + tanh_part) + 0.5 * shifted * (1.0 - tanh_part * tanh_part) * ROOT * (
        1.0 + 3.0 * CUBIC * shifted * shifted
    )


def loop(first, count, step):
    if count <= 4:
        for d in range(first, count):
            step(d)
    else:
        lax.fori_loop(first, count, lambda d, c: (step(d), c)[1], 0)


def others(me, count, step):
    loop(1, count, lambda d: step(lax.rem(me + d, count)))


def signal(barrier, **where):
    pl.semaphore_signal(barrier, inc=1, device_id=where, device_id_type=MESH)


def remote(src, dst, send_sem, recv_sem, **where):
    return pltpu.make_async_remote_copy(
        src_ref=src, dst_ref=dst, send_sem=send_sem, recv_sem=recv_sem, device_id=where,
        device_id_type=MESH,
    )


ANY = pl.BlockSpec(memory_space=pl.ANY)


def bounce(src, dst, held, sem):
    into = pltpu.make_async_copy(src, held, sem)
    into.start()
    into.wait()
    out = pltpu.make_async_copy(held, dst, sem)
    out.start()
    return out


def nearest(l, n, step):
    def both(d):
        for j in (l - d, l + d):

            @pl.when((j >= 0) & (j < n))
            def _():
                step(j)

    loop(1, n, both)


def line_gather(l, n, src, slot, send_sem, recv_sem, arrived):
    def own(step):
        @pl.when(l < n - 1)
        def _():
            step(remote(src, slot(l), send_sem.at[l], recv_sem.at[l], lay=l + 1))

        @pl.when(l > 0)
        def _():
            step(remote(src, slot(l), send_sem.at[n], recv_sem.at[l], lay=l - 1))

    def hop(j, step):
        @pl.when((j < l) & (l < n - 1))
        def _():
            step(remote(slot(j), slot(j), send_sem.at[j], recv_sem.at[j], lay=l + 1))

        @pl.when((j > l) & (l > 0))
        def _():
            step(remote(slot(j), slot(j), send_sem.at[j], recv_sem.at[j], lay=l - 1))

    def take(j):
        remote(slot(j), slot(j), send_sem.at[j], recv_sem.at[j], lay=j).wait_recv()
        hop(j, lambda c: c.start())
        arrived(j)

    def finish():
        own(lambda c: c.wait_send())
        nearest(l, n, lambda j: hop(j, lambda c: c.wait_send()))

    own(lambda c: c.start())
    return lambda: nearest(l, n, take), finish


def comm(body, args, outs, sems, cid, held=()):
    return pl.pallas_call(
        body,
        out_shape=tuple(outs),
        in_specs=[ANY] * len(args),
        out_specs=tuple([ANY] * len(outs)),
        scratch_shapes=[pltpu.SemaphoreType.DMA((s,)) for s in sems] + [pltpu.VMEM(*h) for h in held],
        compiler_params=pltpu.CompilerParams(collective_id=cid, has_side_effects=True),
        name=f"exchange_{cid}",
    )(*args)


def exchange(axis, x, out_shape, held_shape, src_of, dst_of, cid):
    n = lax.axis_size(axis)

    def body(x_ref, o_ref, ssem, rsem, lsem, held):
        me = lax.axis_index(axis)
        barrier = pltpu.get_barrier_semaphore()
        others(me, n, lambda j: signal(barrier, **{axis: j}))
        pl.semaphore_wait(barrier, n - 1)

        def send(j):
            return remote(
                src_of(x_ref, j), dst_of(o_ref, me), ssem.at[j], rsem.at[me], **{axis: j}
            )

        def arrival(j):
            return remote(
                src_of(x_ref, me), dst_of(o_ref, j), ssem.at[j], rsem.at[j], **{axis: j}
            )

        others(me, n, lambda j: send(j).start())
        own = bounce(src_of(x_ref, me), dst_of(o_ref, me), held, lsem.at[0])
        others(me, n, lambda j: arrival(j).wait_recv())
        others(me, n, lambda j: send(j).wait_send())
        own.wait()

    return comm(
        body, [x], [jax.ShapeDtypeStruct(out_shape, x.dtype)], (n, n, 1), cid,
        [(held_shape, x.dtype)],
    )[0]


def gather_errors(e, cid):
    n = lax.axis_size("lay")

    def body(e_ref, o_ref, zs, zr, lsem, held):
        l = lax.axis_index("lay")
        barrier = pltpu.get_barrier_semaphore()
        others(l, n, lambda j: signal(barrier, lay=j))
        pl.semaphore_wait(barrier, n - 1)
        take, finish = line_gather(
            l, n, e_ref, lambda j: o_ref.at[:, j], zs, zr, lambda j: None
        )
        own = bounce(e_ref, o_ref.at[:, l], held, lsem.at[0])
        take()
        finish()
        own.wait()

    out = jax.ShapeDtypeStruct((e.shape[0], n) + e.shape[1:], e.dtype)
    return comm(body, [e], [out], (n + 1, n, 1), cid, [(e.shape, e.dtype)])[0]


def gather_latents(h, cid):
    n, w_count = lax.axis_size("lay"), lax.axis_size("wid")
    blocks, toks, width = h.shape

    def body(h_ref, o_ref, zs, zr, xs, xr, lsem, held):
        l, w = lax.axis_index("lay"), lax.axis_index("wid")
        barrier = pltpu.get_barrier_semaphore()
        others(l, n, lambda j: signal(barrier, lay=j))
        others(w, w_count, lambda v: signal(barrier, wid=v))
        pl.semaphore_wait(barrier, n + w_count - 2)

        def slot(j, v):
            return o_ref.at[pl.ds(j * blocks, blocks), v]

        def x_own(v):
            return remote(h_ref, slot(l, w), xs.at[l * w_count + v], xr.at[l * w_count + w], wid=v)

        def x_copy(j, v, source):
            return remote(
                slot(j, source), slot(j, source), xs.at[j * w_count + v],
                xr.at[j * w_count + source], wid=v,
            )

        take, finish = line_gather(
            l, n, h_ref, lambda j: slot(j, w), zs, zr,
            lambda j: others(w, w_count, lambda v: x_copy(j, v, w).start()),
        )
        others(w, w_count, lambda v: x_own(v).start())
        own = bounce(h_ref, slot(l, w), held, lsem.at[0])
        take()
        finish()
        others(w, w_count, lambda v: x_own(v).wait_send())
        nearest(l, n, lambda j: others(w, w_count, lambda v: x_copy(j, v, w).wait_send()))
        loop(0, n, lambda j: others(w, w_count, lambda v: x_copy(j, v, v).wait_recv()))
        own.wait()

    out = jax.ShapeDtypeStruct((n * blocks, w_count, toks, width), h.dtype)
    return comm(
        body, [h], [out], (n + 1, n, n * w_count, n * w_count, 1), cid, [(h.shape, h.dtype)]
    )[0]


def slots_and_twin(slot_err, lat, err, acts_here, cid):
    w_count, r_count = lax.axis_size("wid"), lax.axis_size("rep")
    assert r_count == 2
    slots, _, toks, width = slot_err.shape
    half = width // r_count

    def body(s_ref, l_ref, e_ref, a_ref, so_ref, lo_ref, eo_ref, ao_ref, ssem, rsem, lsem, ts, tr,
             held, held_acts):
        w, r = lax.axis_index("wid"), lax.axis_index("rep")
        twin = 1 - r
        barrier = pltpu.get_barrier_semaphore()
        others(w, w_count, lambda v: signal(barrier, wid=v))
        signal(barrier, rep=twin)
        pl.semaphore_wait(barrier, w_count)

        def send(v):
            return remote(s_ref.at[:, v], so_ref.at[w], ssem.at[v], rsem.at[w], wid=v)

        def arrival(v):
            return remote(s_ref.at[:, w], so_ref.at[v], ssem.at[v], rsem.at[v], wid=v)

        others(w, w_count, lambda v: send(v).start())
        twins = [
            remote(l_ref.at[:, :, pl.ds(pl.multiple_of(twin * half, half), half)], lo_ref,
                   ts.at[0], tr.at[0], rep=twin),
            remote(e_ref, eo_ref, ts.at[1], tr.at[1], rep=twin),
            remote(a_ref, ao_ref.at[r], ts.at[2], tr.at[2], rep=twin),
        ]
        for c in twins:
            c.start()
        own = bounce(s_ref.at[:, w], so_ref.at[w], held, lsem.at[0])
        own_acts = bounce(a_ref, ao_ref.at[r], held_acts, lsem.at[1])
        others(w, w_count, lambda v: arrival(v).wait_recv())
        others(w, w_count, lambda v: send(v).wait_send())
        own.wait()
        own_acts.wait()
        for c in twins:
            c.wait()

    outs = [
        jax.ShapeDtypeStruct((w_count, slots, toks, width), slot_err.dtype),
        jax.ShapeDtypeStruct(lat.shape[:2] + (half,), lat.dtype),
        jax.ShapeDtypeStruct(err.shape, err.dtype),
        jax.ShapeDtypeStruct((r_count,) + acts_here.shape, acts_here.dtype),
    ]
    return comm(body, [slot_err, lat, err, acts_here], outs, (w_count, w_count, 2, 3, 3), cid,
                [((slots, toks, width), slot_err.dtype), (acts_here.shape, acts_here.dtype)])


def gather_pre_grad(pg, cid):
    w_count, r_count = lax.axis_size("wid"), lax.axis_size("rep")
    _, toks, columns = pg.shape

    def body(p_ref, o_ref, ssem, rsem, lsem, held):
        w, r = lax.axis_index("wid"), lax.axis_index("rep")
        barrier = pltpu.get_barrier_semaphore()

        def peers(step):
            others(w, w_count, lambda v: loop(0, r_count, lambda q: step(v, q)))
            others(r, r_count, lambda q: step(w, q))

        peers(lambda v, q: signal(barrier, wid=v, rep=q))
        pl.semaphore_wait(barrier, w_count * r_count - 1)

        def send(v, q):
            return remote(p_ref.at[q], o_ref.at[r, w], ssem.at[q * w_count + v],
                          rsem.at[r * w_count + w], wid=v, rep=q)

        def arrival(v, q):
            return remote(p_ref.at[q], o_ref.at[q, v], ssem.at[q * w_count + v],
                          rsem.at[q * w_count + v], wid=v, rep=q)

        peers(lambda v, q: send(v, q).start())
        own = bounce(p_ref.at[r], o_ref.at[r, w], held, lsem.at[0])
        peers(lambda v, q: arrival(v, q).wait_recv())
        peers(lambda v, q: send(v, q).wait_send())
        own.wait()

    out = jax.ShapeDtypeStruct((r_count, w_count, toks, columns), pg.dtype)
    total = w_count * r_count
    return comm(
        body, [pg], [out], (total, total, 1), cid, [((toks, columns), pg.dtype)]
    )[0]


def group_of(slots):
    return 3 if slots % 3 == 0 else 1


def slot_call(body, tables, args, in_specs, out_shape, out_spec, scratch, flops, name, grid):
    moved = sum(a.size * a.dtype.itemsize for a in args) + out_shape.size * out_shape.dtype.itemsize
    return pl.pallas_call(
        body,
        out_shape=out_shape,
        grid_spec=pltpu.PrefetchScalarGridSpec(
            num_scalar_prefetch=len(tables), grid=(grid,), in_specs=in_specs,
            out_specs=out_spec, scratch_shapes=scratch,
        ),
        compiler_params=pltpu.CompilerParams(vmem_limit_bytes=62 * 1024 * 1024),
        cost_estimate=pl.CostEstimate(flops=flops, bytes_accessed=moved, transcendentals=0),
        name=name,
    )(*tables, *args)


def decode(ids, tgt, valid, lat, dec_weight, layers):
    slots, block, width = dec_weight.shape
    blocks, toks, _ = lat.shape
    g = group_of(slots)

    def body(i_ref, t_ref, v_ref, lat_ref, w_ref, o_ref, acc):
        step = pl.program_id(0)

        @pl.when(step == 0)
        def _():
            acc[...] = jnp.zeros_like(acc)

        for i in range(g):
            k = step * g + i

            @pl.when(v_ref[k] > 0)
            def _():
                acc[t_ref[k]] += jnp.dot(
                    lat_ref[i_ref[k]], w_ref[i], preferred_element_type=F32
                )

        @pl.when(step == slots // g - 1)
        def _():
            o_ref[...] = acc[...].astype(o_ref.dtype)

    return slot_call(
        body, (ids, tgt, valid), (lat, dec_weight),
        [pl.BlockSpec((blocks, toks, block), lambda k, i, t, v: (0, 0, 0)),
         pl.BlockSpec((g, block, width), lambda k, i, t, v: (k, 0, 0))],
        jax.ShapeDtypeStruct((layers, toks, width), BF16),
        pl.BlockSpec((layers, toks, width), lambda k, i, t, v: (0, 0, 0)),
        [pltpu.VMEM((layers, toks, width), F32)], 2 * slots * toks * block * width, "decode",
        slots // g,
    )


def slot_errors(tgt, err, dec_weight):
    slots, block, width = dec_weight.shape
    layers, toks, _ = err.shape
    g = group_of(slots)

    def body(t_ref, e_ref, w_ref, o_ref):
        for i in range(g):
            k = pl.program_id(0) * g + i
            o_ref[i] = lax.dot_general(
                e_ref[t_ref[k]], w_ref[i], (((1,), (1,)), ((), ())), preferred_element_type=F32
            ).astype(o_ref.dtype)

    return slot_call(
        body, (tgt,), (err, dec_weight),
        [pl.BlockSpec((layers, toks, width), lambda k, t: (0, 0, 0)),
         pl.BlockSpec((g, block, width), lambda k, t: (k, 0, 0))],
        jax.ShapeDtypeStruct((slots, toks, block), BF16),
        pl.BlockSpec((g, toks, block), lambda k, t: (k, 0, 0)),
        [], 2 * slots * toks * block * width, "slot_errors", slots // g,
    )


def combine(ids, valid, parts, blocks_total):
    w_count, slots, toks, block = parts.shape

    g = slots // 3 if slots % 3 == 0 else 1

    def body(i_ref, v_ref, p_ref, o_ref, acc):
        step = pl.program_id(0)

        @pl.when(step == 0)
        def _():
            acc[...] = jnp.zeros_like(acc)

        for i in range(g):
            k = step * g + i

            @pl.when(v_ref[k] > 0)
            def _():
                acc[i_ref[k]] += jnp.sum(p_ref[:, i].astype(F32), axis=0)

        @pl.when(step == slots // g - 1)
        def _():
            o_ref[...] = acc[...].astype(o_ref.dtype)

    return slot_call(
        body, (ids, valid), (parts,),
        [pl.BlockSpec((w_count, g, toks, block), lambda k, i, v: (0, k, 0, 0))],
        jax.ShapeDtypeStruct((blocks_total, toks, block), BF16),
        pl.BlockSpec((blocks_total, toks, block), lambda k, i, v: (0, 0, 0)),
        [pltpu.VMEM((blocks_total, toks, block), F32)], w_count * slots * toks * block, "combine",
        slots // g,
    )


def decoder_grads(ids, tgt, valid, rep, lat, lat_twin, err, err_twin, slots):
    layers, toks, width = err.shape
    blocks, _, half = lat_twin.shape
    g = group_of(slots)

    def body(i_ref, t_ref, v_ref, r_ref, l_ref, lt_ref, e_ref, et_ref, o_ref):
        over = (((0,), (0,)), ((), ()))
        for i in range(g):
            k = pl.program_id(0) * g + i

            @pl.when(v_ref[k] > 0)
            def _():
                t, b = t_ref[k], i_ref[k]
                o_ref[i] = lax.dot_general(
                    l_ref[b], e_ref[t], over, preferred_element_type=F32
                ) + lax.dot_general(lt_ref[b], et_ref[t], over, preferred_element_type=F32)

            @pl.when(v_ref[k] == 0)
            def _():
                o_ref[i] = jnp.zeros_like(o_ref[i])

    return slot_call(
        body, (ids, tgt, valid, rep), (lat, lat_twin, err, err_twin),
        [pl.BlockSpec((blocks, toks, half), lambda k, i, t, v, r: (0, 0, r[0])),
         pl.BlockSpec((blocks, toks, half), lambda k, i, t, v, r: (0, 0, 0)),
         pl.BlockSpec((layers, toks, width), lambda k, i, t, v, r: (0, 0, 0)),
         pl.BlockSpec((layers, toks, width), lambda k, i, t, v, r: (0, 0, 0))],
        jax.ShapeDtypeStruct((slots, half, width), F32),
        pl.BlockSpec((g, half, width), lambda k, i, t, v, r: (k, 0, 0)),
        [], 4 * slots * toks * half * width, "decoder_grads", slots // g,
    )


def local(acts, targets, enc_weight, enc_bias, gate_mask, dec_list, dec_weight):
    layers, tok_rows, width_part = acts.shape
    lat_dev = enc_weight.shape[1]
    slots, block, _ = dec_weight.shape
    per_dev = lat_dev // block
    n, w_count, r_count = lax.axis_size("lay"), lax.axis_size("wid"), lax.axis_size("rep")
    lay, wid, rep = lax.axis_index("lay"), lax.axis_index("wid"), lax.axis_index("rep")
    lat_total = lat_dev * n
    blocks_total = lat_total // block
    latents_layer = lat_total // layers
    blocks_layer = latents_layer // block
    toks = tok_rows // w_count
    rows = tok_rows // n

    tgt = dec_list[:, 1]
    valid = (tgt >= 0).astype(jnp.int32)
    ids = jnp.maximum(dec_list[:, 0] * blocks_layer + dec_list[:, 2], 0)
    tgt = jnp.maximum(tgt, 0)

    here = lax.dynamic_index_in_dim(acts, lay * lat_dev // latents_layer, 0, keepdims=False)
    partial = jnp.dot(here, enc_weight, preferred_element_type=F32).astype(BF16)
    parts = exchange(
        "wid", partial.reshape(w_count, toks, lat_dev), (w_count, toks, lat_dev), (toks, lat_dev),
        lambda x, j: x.at[j], lambda o, j: o.at[j], 0,
    )
    shifted = jnp.sum(parts.astype(F32), axis=0) + enc_bias[None, :]
    shifted = shifted.reshape(toks, per_dev, block).transpose(1, 0, 2)
    keep = lax.dynamic_slice_in_dim(gate_mask, wid * toks, toks, 0).astype(F32).T[:, :, None]
    latent = (smooth_gate(shifted) * keep).astype(BF16)
    lat = gather_latents(latent, 1).reshape(blocks_total, tok_rows, block)

    recon_part = decode(ids, tgt, valid, lat, dec_weight, layers)
    recon_in = exchange(
        "lay", recon_part.reshape(layers, n, rows, width_part), (n, layers, rows, width_part),
        (layers, rows, width_part), lambda x, j: x.at[:, j], lambda o, j: o.at[j], 2,
    )
    recon = jnp.sum(recon_in.astype(F32), axis=0)
    own_target = lax.dynamic_slice_in_dim(targets, lay * rows, rows, 1)
    scale = float(tok_rows * r_count) ** (-0.5)
    own_err = ((recon - own_target.astype(F32)) * scale).astype(BF16)
    err = gather_errors(own_err, 3).reshape(layers, tok_rows, width_part)

    slot_err = slot_errors(tgt, err, dec_weight).reshape(slots, w_count, toks, block)
    slot_in, lat_twin, err_twin, acts_all = slots_and_twin(slot_err, lat, err, here, 4)
    outgoing = combine(ids, valid, slot_in, blocks_total)
    incoming = exchange(
        "lay", outgoing.reshape(n, per_dev, toks, block), (n, per_dev, toks, block),
        (per_dev, toks, block), lambda x, j: x.at[j], lambda o, j: o.at[j], 5,
    )
    dec_out = decoder_grads(
        ids, tgt, valid, rep.reshape(1).astype(jnp.int32), lat, lat_twin, err, err_twin, slots
    )
    latent_error = jnp.sum(incoming.astype(F32), axis=0)
    pre_grad = (latent_error * keep * gate_slope(shifted)).astype(BF16)
    columns = lat_dev // r_count
    pre_grad = pre_grad.transpose(1, 0, 2).reshape(toks, r_count, columns).transpose(1, 0, 2)
    pre_all = gather_pre_grad(pre_grad, 6).reshape(r_count, tok_rows, columns)

    enc_out = lax.dot_general(
        acts_all.reshape(r_count * tok_rows, width_part),
        pre_all.reshape(r_count * tok_rows, columns), (((0,), (0,)), ((), ())),
        preferred_element_type=F32,
    )
    bias_out = jnp.sum(pre_all.astype(F32), axis=(0, 1))
    return (enc_out, bias_out, dec_out)


def solution(mesh):
    return jax.shard_map(
        local,
        mesh=mesh,
        in_specs=(
            P(None, ("grp", "rep"), "wid"),
            P(None, ("grp", "rep"), "wid"),
            P("wid", "lay"),
            P("lay"),
            P(("grp", "rep"), "lay"),
            P("lay", None),
            P("lay", None, "wid"),
        ),
        out_specs=(
            P(("grp", "wid"), ("lay", "rep")),
            P(("grp", "lay", "rep")),
            P(("grp", "lay"), "rep", "wid"),
        ),
        check_vma=False,
    )
```

```python
import jax
import jax.numpy as jnp
from jax import lax
from jax.experimental import pallas as pl
from jax.experimental.pallas import tpu as pltpu
from jax.sharding import PartitionSpec as P

ROOT = 0.7978845608028654
CUBIC = 0.044715
MESH = pl.DeviceIdType.MESH
BF16 = jnp.bfloat16
F32 = jnp.float32


def smooth_gate(shifted):
    inside_arg = ROOT * (shifted + CUBIC * shifted * shifted * shifted)
    return 0.5 * shifted * (1.0 + jnp.tanh(inside_arg))


def gate_slope(shifted):
    inside_arg = ROOT * (shifted + CUBIC * shifted * shifted * shifted)
    tanh_part = jnp.tanh(inside_arg)
    return 0.5 * (1.0 + tanh_part) + 0.5 * shifted * (1.0 - tanh_part * tanh_part) * ROOT * (
        1.0 + 3.0 * CUBIC * shifted * shifted
    )


def loop(first, count, step):
    if count <= 4:
        for d in range(first, count):
            step(d)
    else:
        lax.fori_loop(first, count, lambda d, c: (step(d), c)[1], 0)


def others(me, count, step):
    loop(1, count, lambda d: step(lax.rem(me + d, count)))


def signal(barrier, **where):
    pl.semaphore_signal(barrier, inc=1, device_id=where, device_id_type=MESH)


def remote(src, dst, send_sem, recv_sem, **where):
    return pltpu.make_async_remote_copy(
        src_ref=src, dst_ref=dst, send_sem=send_sem, recv_sem=recv_sem, device_id=where,
        device_id_type=MESH,
    )


ANY = pl.BlockSpec(memory_space=pl.ANY)


def bounce(src, dst, held, sem):
    into = pltpu.make_async_copy(src, held, sem)
    into.start()
    into.wait()
    out = pltpu.make_async_copy(held, dst, sem)
    out.start()
    return out


def nearest(l, n, step):
    def both(d):
        for j in (l - d, l + d):

            @pl.when((j >= 0) & (j < n))
            def _():
                step(j)

    loop(1, n, both)


def line_gather(l, n, src, slot, send_sem, recv_sem, arrived):
    def own(step):
        @pl.when(l < n - 1)
        def _():
            step(remote(src, slot(l), send_sem.at[l], recv_sem.at[l], lay=l + 1))

        @pl.when(l > 0)
        def _():
            step(remote(src, slot(l), send_sem.at[n], recv_sem.at[l], lay=l - 1))

    def hop(j, step):
        @pl.when((j < l) & (l < n - 1))
        def _():
            step(remote(slot(j), slot(j), send_sem.at[j], recv_sem.at[j], lay=l + 1))

        @pl.when((j > l) & (l > 0))
        def _():
            step(remote(slot(j), slot(j), send_sem.at[j], recv_sem.at[j], lay=l - 1))

    def take(j):
        remote(slot(j), slot(j), send_sem.at[j], recv_sem.at[j], lay=j).wait_recv()
        hop(j, lambda c: c.start())
        arrived(j)

    def finish():
        own(lambda c: c.wait_send())
        nearest(l, n, lambda j: hop(j, lambda c: c.wait_send()))

    own(lambda c: c.start())
    return lambda: nearest(l, n, take), finish


def comm(body, args, outs, sems, cid, held=()):
    return pl.pallas_call(
        body,
        out_shape=tuple(outs),
        in_specs=[ANY] * len(args),
        out_specs=tuple([ANY] * len(outs)),
        scratch_shapes=[pltpu.SemaphoreType.DMA((s,)) for s in sems] + [pltpu.VMEM(*h) for h in held],
        compiler_params=pltpu.CompilerParams(collective_id=cid, has_side_effects=True),
        name=f"exchange_{cid}",
    )(*args)


def exchange(axis, x, out_shape, held_shape, src_of, dst_of, cid):
    n = lax.axis_size(axis)

    def body(x_ref, o_ref, ssem, rsem, lsem, held):
        me = lax.axis_index(axis)
        barrier = pltpu.get_barrier_semaphore()
        others(me, n, lambda j: signal(barrier, **{axis: j}))
        pl.semaphore_wait(barrier, n - 1)

        def send(j):
            return remote(
                src_of(x_ref, j), dst_of(o_ref, me), ssem.at[j], rsem.at[me], **{axis: j}
            )

        def arrival(j):
            return remote(
                src_of(x_ref, me), dst_of(o_ref, j), ssem.at[j], rsem.at[j], **{axis: j}
            )

        others(me, n, lambda j: send(j).start())
        own = bounce(src_of(x_ref, me), dst_of(o_ref, me), held, lsem.at[0])
        others(me, n, lambda j: arrival(j).wait_recv())
        others(me, n, lambda j: send(j).wait_send())
        own.wait()

    return comm(
        body, [x], [jax.ShapeDtypeStruct(out_shape, x.dtype)], (n, n, 1), cid,
        [(held_shape, x.dtype)],
    )[0]


def gather_errors(e, cid):
    n = lax.axis_size("lay")

    def body(e_ref, o_ref, zs, zr, lsem, held):
        l = lax.axis_index("lay")
        barrier = pltpu.get_barrier_semaphore()
        others(l, n, lambda j: signal(barrier, lay=j))
        pl.semaphore_wait(barrier, n - 1)
        take, finish = line_gather(
            l, n, e_ref, lambda j: o_ref.at[:, j], zs, zr, lambda j: None
        )
        own = bounce(e_ref, o_ref.at[:, l], held, lsem.at[0])
        take()
        finish()
        own.wait()

    out = jax.ShapeDtypeStruct((e.shape[0], n) + e.shape[1:], e.dtype)
    return comm(body, [e], [out], (n + 1, n, 1), cid, [(e.shape, e.dtype)])[0]


def gather_latents(h, cid):
    n, w_count = lax.axis_size("lay"), lax.axis_size("wid")
    blocks, toks, width = h.shape

    def body(h_ref, o_ref, zs, zr, xs, xr, lsem, held):
        l, w = lax.axis_index("lay"), lax.axis_index("wid")
        barrier = pltpu.get_barrier_semaphore()
        others(l, n, lambda j: signal(barrier, lay=j))
        others(w, w_count, lambda v: signal(barrier, wid=v))
        pl.semaphore_wait(barrier, n + w_count - 2)

        def slot(j, v):
            return o_ref.at[pl.ds(j * blocks, blocks), v]

        def x_own(v):
            return remote(h_ref, slot(l, w), xs.at[l * w_count + v], xr.at[l * w_count + w], wid=v)

        def x_copy(j, v, source):
            return remote(
                slot(j, source), slot(j, source), xs.at[j * w_count + v],
                xr.at[j * w_count + source], wid=v,
            )

        take, finish = line_gather(
            l, n, h_ref, lambda j: slot(j, w), zs, zr,
            lambda j: others(w, w_count, lambda v: x_copy(j, v, w).start()),
        )
        others(w, w_count, lambda v: x_own(v).start())
        own = bounce(h_ref, slot(l, w), held, lsem.at[0])
        take()
        finish()
        others(w, w_count, lambda v: x_own(v).wait_send())
        nearest(l, n, lambda j: others(w, w_count, lambda v: x_copy(j, v, w).wait_send()))
        loop(0, n, lambda j: others(w, w_count, lambda v: x_copy(j, v, v).wait_recv()))
        own.wait()

    out = jax.ShapeDtypeStruct((n * blocks, w_count, toks, width), h.dtype)
    return comm(
        body, [h], [out], (n + 1, n, n * w_count, n * w_count, 1), cid, [(h.shape, h.dtype)]
    )[0]


def slots_and_twin(slot_err, lat, err, acts_here, cid):
    w_count, r_count = lax.axis_size("wid"), lax.axis_size("rep")
    assert r_count == 2
    slots, _, toks, width = slot_err.shape
    half = width // r_count

    def body(s_ref, l_ref, e_ref, a_ref, so_ref, lo_ref, eo_ref, ao_ref, ssem, rsem, lsem, ts, tr,
             held, held_acts):
        w, r = lax.axis_index("wid"), lax.axis_index("rep")
        twin = 1 - r
        barrier = pltpu.get_barrier_semaphore()
        others(w, w_count, lambda v: signal(barrier, wid=v))
        signal(barrier, rep=twin)
        pl.semaphore_wait(barrier, w_count)

        def send(v):
            return remote(s_ref.at[:, v], so_ref.at[w], ssem.at[v], rsem.at[w], wid=v)

        def arrival(v):
            return remote(s_ref.at[:, w], so_ref.at[v], ssem.at[v], rsem.at[v], wid=v)

        others(w, w_count, lambda v: send(v).start())
        twins = [
            remote(l_ref.at[:, :, pl.ds(pl.multiple_of(twin * half, half), half)], lo_ref,
                   ts.at[0], tr.at[0], rep=twin),
            remote(e_ref, eo_ref, ts.at[1], tr.at[1], rep=twin),
            remote(a_ref, ao_ref.at[r], ts.at[2], tr.at[2], rep=twin),
        ]
        for c in twins:
            c.start()
        own = bounce(s_ref.at[:, w], so_ref.at[w], held, lsem.at[0])
        own_acts = bounce(a_ref, ao_ref.at[r], held_acts, lsem.at[1])
        others(w, w_count, lambda v: arrival(v).wait_recv())
        others(w, w_count, lambda v: send(v).wait_send())
        own.wait()
        own_acts.wait()
        for c in twins:
            c.wait()

    outs = [
        jax.ShapeDtypeStruct((w_count, slots, toks, width), slot_err.dtype),
        jax.ShapeDtypeStruct(lat.shape[:2] + (half,), lat.dtype),
        jax.ShapeDtypeStruct(err.shape, err.dtype),
        jax.ShapeDtypeStruct((r_count,) + acts_here.shape, acts_here.dtype),
    ]
    return comm(body, [slot_err, lat, err, acts_here], outs, (w_count, w_count, 2, 3, 3), cid,
                [((slots, toks, width), slot_err.dtype), (acts_here.shape, acts_here.dtype)])


def gather_pre_grad(pg, cid):
    w_count, r_count = lax.axis_size("wid"), lax.axis_size("rep")
    _, toks, columns = pg.shape

    def body(p_ref, o_ref, ssem, rsem, lsem, held):
        w, r = lax.axis_index("wid"), lax.axis_index("rep")
        barrier = pltpu.get_barrier_semaphore()

        def peers(step):
            others(w, w_count, lambda v: loop(0, r_count, lambda q: step(v, q)))
            others(r, r_count, lambda q: step(w, q))

        peers(lambda v, q: signal(barrier, wid=v, rep=q))
        pl.semaphore_wait(barrier, w_count * r_count - 1)

        def send(v, q):
            return remote(p_ref.at[q], o_ref.at[r, w], ssem.at[q * w_count + v],
                          rsem.at[r * w_count + w], wid=v, rep=q)

        def arrival(v, q):
            return remote(p_ref.at[q], o_ref.at[q, v], ssem.at[q * w_count + v],
                          rsem.at[q * w_count + v], wid=v, rep=q)

        peers(lambda v, q: send(v, q).start())
        own = bounce(p_ref.at[r], o_ref.at[r, w], held, lsem.at[0])
        peers(lambda v, q: arrival(v, q).wait_recv())
        peers(lambda v, q: send(v, q).wait_send())
        own.wait()

    out = jax.ShapeDtypeStruct((r_count, w_count, toks, columns), pg.dtype)
    total = w_count * r_count
    return comm(
        body, [pg], [out], (total, total, 1), cid, [((toks, columns), pg.dtype)]
    )[0]


def group_of(slots):
    return 3 if slots % 3 == 0 else 1


def slot_call(body, tables, args, in_specs, out_shape, out_spec, scratch, flops, name, grid):
    moved = sum(a.size * a.dtype.itemsize for a in args) + out_shape.size * out_shape.dtype.itemsize
    return pl.pallas_call(
        body,
        out_shape=out_shape,
        grid_spec=pltpu.PrefetchScalarGridSpec(
            num_scalar_prefetch=len(tables), grid=(grid,), in_specs=in_specs,
            out_specs=out_spec, scratch_shapes=scratch,
        ),
        compiler_params=pltpu.CompilerParams(vmem_limit_bytes=62 * 1024 * 1024),
        cost_estimate=pl.CostEstimate(flops=flops, bytes_accessed=moved, transcendentals=0),
        name=name,
    )(*tables, *args)


def decode(ids, tgt, valid, lat, dec_weight, layers):
    slots, block, width = dec_weight.shape
    blocks, toks, _ = lat.shape
    g = group_of(slots)

    def body(i_ref, t_ref, v_ref, lat_ref, w_ref, o_ref, acc):
        step = pl.program_id(0)

        @pl.when(step == 0)
        def _():
            acc[...] = jnp.zeros_like(acc)

        for i in range(g):
            k = step * g + i

            @pl.when(v_ref[k] > 0)
            def _():
                acc[t_ref[k]] += jnp.dot(
                    lat_ref[i_ref[k]], w_ref[i], preferred_element_type=F32
                )

        @pl.when(step == slots // g - 1)
        def _():
            o_ref[...] = acc[...].astype(o_ref.dtype)

    return slot_call(
        body, (ids, tgt, valid), (lat, dec_weight),
        [pl.BlockSpec((blocks, toks, block), lambda k, i, t, v: (0, 0, 0)),
         pl.BlockSpec((g, block, width), lambda k, i, t, v: (k, 0, 0))],
        jax.ShapeDtypeStruct((layers, toks, width), BF16),
        pl.BlockSpec((layers, toks, width), lambda k, i, t, v: (0, 0, 0)),
        [pltpu.VMEM((layers, toks, width), F32)], 2 * slots * toks * block * width, "decode",
        slots // g,
    )


def slot_errors(tgt, err, dec_weight):
    slots, block, width = dec_weight.shape
    layers, toks, _ = err.shape
    g = group_of(slots)

    def body(t_ref, e_ref, w_ref, o_ref):
        for i in range(g):
            k = pl.program_id(0) * g + i
            o_ref[i] = lax.dot_general(
                e_ref[t_ref[k]], w_ref[i], (((1,), (1,)), ((), ())), preferred_element_type=F32
            ).astype(o_ref.dtype)

    return slot_call(
        body, (tgt,), (err, dec_weight),
        [pl.BlockSpec((layers, toks, width), lambda k, t: (0, 0, 0)),
         pl.BlockSpec((g, block, width), lambda k, t: (k, 0, 0))],
        jax.ShapeDtypeStruct((slots, toks, block), BF16),
        pl.BlockSpec((g, toks, block), lambda k, t: (k, 0, 0)),
        [], 2 * slots * toks * block * width, "slot_errors", slots // g,
    )


def combine(ids, valid, parts, blocks_total):
    w_count, slots, toks, block = parts.shape

    g = slots // 3 if slots % 3 == 0 else 1

    def body(i_ref, v_ref, p_ref, o_ref, acc):
        step = pl.program_id(0)

        @pl.when(step == 0)
        def _():
            acc[...] = jnp.zeros_like(acc)

        for i in range(g):
            k = step * g + i

            @pl.when(v_ref[k] > 0)
            def _():
                acc[i_ref[k]] += jnp.sum(p_ref[:, i].astype(F32), axis=0)

        @pl.when(step == slots // g - 1)
        def _():
            o_ref[...] = acc[...].astype(o_ref.dtype)

    return slot_call(
        body, (ids, valid), (parts,),
        [pl.BlockSpec((w_count, g, toks, block), lambda k, i, v: (0, k, 0, 0))],
        jax.ShapeDtypeStruct((blocks_total, toks, block), BF16),
        pl.BlockSpec((blocks_total, toks, block), lambda k, i, v: (0, 0, 0)),
        [pltpu.VMEM((blocks_total, toks, block), F32)], w_count * slots * toks * block, "combine",
        slots // g,
    )


def decoder_grads(ids, tgt, valid, rep, lat, lat_twin, err, err_twin, slots):
    layers, toks, width = err.shape
    blocks, _, half = lat_twin.shape
    g = group_of(slots)

    def body(i_ref, t_ref, v_ref, r_ref, l_ref, lt_ref, e_ref, et_ref, o_ref):
        over = (((0,), (0,)), ((), ()))
        for i in range(g):
            k = pl.program_id(0) * g + i

            @pl.when(v_ref[k] > 0)
            def _():
                t, b = t_ref[k], i_ref[k]
                o_ref[i] = lax.dot_general(
                    l_ref[b], e_ref[t], over, preferred_element_type=F32
                ) + lax.dot_general(lt_ref[b], et_ref[t], over, preferred_element_type=F32)

            @pl.when(v_ref[k] == 0)
            def _():
                o_ref[i] = jnp.zeros_like(o_ref[i])

    return slot_call(
        body, (ids, tgt, valid, rep), (lat, lat_twin, err, err_twin),
        [pl.BlockSpec((blocks, toks, half), lambda k, i, t, v, r: (0, 0, r[0])),
         pl.BlockSpec((blocks, toks, half), lambda k, i, t, v, r: (0, 0, 0)),
         pl.BlockSpec((layers, toks, width), lambda k, i, t, v, r: (0, 0, 0)),
         pl.BlockSpec((layers, toks, width), lambda k, i, t, v, r: (0, 0, 0))],
        jax.ShapeDtypeStruct((slots, half, width), F32),
        pl.BlockSpec((g, half, width), lambda k, i, t, v, r: (k, 0, 0)),
        [], 4 * slots * toks * half * width, "decoder_grads", slots // g,
    )


def local(acts, targets, enc_weight, enc_bias, gate_mask, dec_list, dec_weight):
    layers, tok_rows, width_part = acts.shape
    lat_dev = enc_weight.shape[1]
    slots, block, _ = dec_weight.shape
    per_dev = lat_dev // block
    n, w_count, r_count = lax.axis_size("lay"), lax.axis_size("wid"), lax.axis_size("rep")
    lay, wid, rep = lax.axis_index("lay"), lax.axis_index("wid"), lax.axis_index("rep")
    lat_total = lat_dev * n
    blocks_total = lat_total // block
    latents_layer = lat_total // layers
    blocks_layer = latents_layer // block
    toks = tok_rows // w_count
    rows = tok_rows // n

    tgt = dec_list[:, 1]
    valid = (tgt >= 0).astype(jnp.int32)
    ids = jnp.maximum(dec_list[:, 0] * blocks_layer + dec_list[:, 2], 0)
    tgt = jnp.maximum(tgt, 0)

    here = lax.dynamic_index_in_dim(acts, lay * lat_dev // latents_layer, 0, keepdims=False)
    partial = jnp.dot(here, enc_weight, preferred_element_type=F32).astype(BF16)
    parts = exchange(
        "wid", partial.reshape(w_count, toks, lat_dev), (w_count, toks, lat_dev), (toks, lat_dev),
        lambda x, j: x.at[j], lambda o, j: o.at[j], 0,
    )
    shifted = jnp.sum(parts.astype(F32), axis=0) + enc_bias[None, :]
    shifted = shifted.reshape(toks, per_dev, block).transpose(1, 0, 2)
    keep = lax.dynamic_slice_in_dim(gate_mask, wid * toks, toks, 0).astype(F32).T[:, :, None]
    latent = (smooth_gate(shifted) * keep).astype(BF16)
    lat = gather_latents(latent, 1).reshape(blocks_total, tok_rows, block)

    recon_part = decode(ids, tgt, valid, lat, dec_weight, layers)
    recon_in = exchange(
        "lay", recon_part.reshape(layers, n, rows, width_part), (n, layers, rows, width_part),
        (layers, rows, width_part), lambda x, j: x.at[:, j], lambda o, j: o.at[j], 2,
    )
    recon = jnp.sum(recon_in.astype(F32), axis=0)
    own_target = lax.dynamic_slice_in_dim(targets, lay * rows, rows, 1)
    scale = float(tok_rows * r_count) ** (-0.5)
    own_err = ((recon - own_target.astype(F32)) * scale).astype(BF16)
    err = gather_errors(own_err, 3).reshape(layers, tok_rows, width_part)

    slot_err = slot_errors(tgt, err, dec_weight).reshape(slots, w_count, toks, block)
    slot_in, lat_twin, err_twin, acts_all = slots_and_twin(slot_err, lat, err, here, 4)
    outgoing = combine(ids, valid, slot_in, blocks_total)
    outgoing = outgoing.reshape(n, per_dev, toks, block)
    incoming = [lax.dynamic_index_in_dim(outgoing, lay, 0, keepdims=False)]
    for d in range(1, n):
        part = lax.dynamic_index_in_dim(outgoing, lax.rem(lay + d, n), 0, keepdims=False)
        incoming.append(lax.ppermute(part, "lay", [(i, (i + d) % n) for i in range(n)]))
    dec_out = decoder_grads(
        ids, tgt, valid, rep.reshape(1).astype(jnp.int32), lat, lat_twin, err, err_twin, slots
    )
    latent_error = sum(part.astype(F32) for part in incoming)
    pre_grad = (latent_error * keep * gate_slope(shifted)).astype(BF16)
    columns = lat_dev // r_count
    pre_grad = pre_grad.transpose(1, 0, 2).reshape(toks, r_count, columns).transpose(1, 0, 2)
    pre_all = gather_pre_grad(pre_grad, 6).reshape(r_count, tok_rows, columns)

    enc_out = lax.dot_general(
        acts_all.reshape(r_count * tok_rows, width_part),
        pre_all.reshape(r_count * tok_rows, columns), (((0,), (0,)), ((), ())),
        preferred_element_type=F32,
    )
    bias_out = jnp.sum(pre_all.astype(F32), axis=(0, 1))
    return (enc_out, bias_out, dec_out)


def solution(mesh):
    return jax.shard_map(
        local,
        mesh=mesh,
        in_specs=(
            P(None, ("grp", "rep"), "wid"),
            P(None, ("grp", "rep"), "wid"),
            P("wid", "lay"),
            P("lay"),
            P(("grp", "rep"), "lay"),
            P("lay", None),
            P("lay", None, "wid"),
        ),
        out_specs=(
            P(("grp", "wid"), ("lay", "rep")),
            P(("grp", "lay", "rep")),
            P(("grp", "lay"), "rep", "wid"),
        ),
        check_vma=False,
    )
```
